32 devices in a mesh: section: 4 (over y, core), seq: 8 (over z, x).
Axes of the slice: x: 2, y: 2, z: 4, core: 2. Of those that a mesh axis runs over, the one named last changes fastest.
Arguments:
- stream: bfloat16 [4, 512, 1024], P('section', 'seq'), may hold values from -1.5 to 1.5
- queries: bfloat16 [4, 512, 1024], P('section', 'seq'), may hold values from -8 to 8
- key_rows: bfloat16 [4, 512, 1024], P('section', 'seq'), may hold values from -8 to 8
- values: bfloat16 [4, 512, 1024], P('section', 'seq'), may hold values from -36 to 36
- incoming: bfloat16 [512, 1024], P('seq'), may hold values from -1.5 to 1.5
Outputs:
- updated: bfloat16 [4, 512, 1024], P('section', 'seq')
- received: bfloat16 [4, 512, 1024], P('section', 'seq')
The draws below stay inside these ranges and needn't reach their ends.
All inputs are finite; a program needn't handle non-finite values.
Results may differ from the reference program's by a relative error of at most 0.0054.
Values may be sent and summed in bfloat16 or wider, within the bound.
A program may use at most 64 MiB of HBM per device.

```python
import jax
import jax.numpy as jnp
from jax import lax

HEAD_SIZE = 128
D = 1024
TOKENS = 512
SEQ_LEN = 512
SEQS = 1
SECTIONS = 4


def make_pair(key):
    shape = (SECTIONS, TOKENS, D)
    query_key = jax.random.fold_in(key, 101)
    other_key = jax.random.fold_in(key, 102)
    queries = jnp.clip(jax.random.normal(query_key, shape, jnp.float32), -6.0, 6.0)
    keys_all = jnp.clip(jax.random.normal(other_key, shape, jnp.float32), -6.0, 6.0)
    return (queries, keys_all)


def draw_queries(key, part):
    return make_pair(key)[0].astype(jnp.bfloat16)


def draw_key_rows(key, part):
    return make_pair(key)[1].astype(jnp.bfloat16)


def steps_of(key, extent, shards, smallest, largest):
    gain, own = 1.0, jax.random.fold_in(key, 6)
    for dim, blocks in shards:
        steps = jnp.exp(jax.random.uniform(jax.random.fold_in(own, dim), (blocks,), jnp.float32, smallest / len(shards), largest / len(shards)))
        gain = gain * jnp.repeat(steps, extent[dim] // blocks).reshape([-1 if axis == dim else 1 for axis in range(len(extent))])
    return gain


def gaussian(rng, shape, deviation, limit, cuts=(), held_as=jnp.bfloat16):
    drawn = jax.random.normal(rng, shape, jnp.float32) * deviation
    if len(cuts) > 0:
        drawn = steps_of(rng, shape, cuts, -0.22, 0.18) * drawn
    return jnp.clip(drawn, min=-limit, max=limit).astype(held_as)


def setup_inputs(seed: int = 0) -> dict:
    key_of = jax.random.split(jax.random.key(seed), 6)
    return {
        "stream": gaussian(key_of[0], (SECTIONS, TOKENS, D), 0.25, 1.5, ((0, 4), (1, 8))),
        "queries": draw_queries(jax.random.fold_in(key_of[5], 71), 0),
        "key_rows": draw_key_rows(jax.random.fold_in(key_of[5], 71), 0),
        "values": gaussian(key_of[3], (SECTIONS, TOKENS, D), 6.0, 36.0, ((0, 4), (1, 8))),
        "incoming": gaussian(key_of[4], (TOKENS, D), 0.25, 1.5, ((0, 8),)),
    }


def attend_sequence(pieces):
    query_rows, key_rows, value_rows = pieces
    tok_count = query_rows.shape[0]
    head_count = query_rows.shape[1] // HEAD_SIZE
    query_f = query_rows.astype(jnp.float32).reshape(tok_count, head_count, HEAD_SIZE)
    key_f = key_rows.astype(jnp.float32).reshape(tok_count, head_count, HEAD_SIZE)
    value_f = value_rows.astype(jnp.float32).reshape(tok_count, head_count, HEAD_SIZE)
    scale = HEAD_SIZE ** -0.5
    scores = jnp.einsum("qhd,khd->hqk", query_f, key_f) * scale
    highest = jnp.max(scores, axis=-1, keepdims=True)
    exponent = jnp.exp(scores - highest)
    totals = jnp.sum(exponent, axis=-1)
    weights = lax.optimization_barrier(exponent.astype(jnp.bfloat16)).astype(jnp.float32)
    summed = jnp.einsum("hqk,khd->qhd", weights, value_f)
    attended = (summed / jnp.transpose(totals)[:, :, None]).astype(jnp.bfloat16)
    return attended.reshape(tok_count, head_count * HEAD_SIZE)


def attend_section(pieces):
    query_rows, key_rows, value_rows, stream_rows = pieces
    width = query_rows.shape[1]
    query_seq = query_rows.reshape(SEQS, SEQ_LEN, width)
    key_seq = key_rows.reshape(SEQS, SEQ_LEN, width)
    value_seq = value_rows.reshape(SEQS, SEQ_LEN, width)
    attended = lax.map(attend_sequence, (query_seq, key_seq, value_seq)).reshape(TOKENS, width)
    return (stream_rows.astype(jnp.float32) + attended.astype(jnp.float32)).astype(jnp.bfloat16)


def reference(stream, queries, key_rows, values, incoming):
    updated = lax.map(attend_section, (queries, key_rows, values, stream))
    received = jnp.concatenate([incoming[None], updated[:-1]], axis=0)
    return updated, received
```

```python
import functools

import jax
import jax.numpy as jnp
from jax import lax
from jax.experimental import pallas as pl
from jax.experimental.pallas import tpu as pltpu
from jax.sharding import PartitionSpec as P

HEAD_SIZE = 128
GROUP = 8
LOG2_E = 1.4426950408889634
MESH = pl.DeviceIdType.MESH


def flipped(place, mask):
    result, weight = 0, 1
    while weight < GROUP:
        bit = lax.rem(lax.div(place, weight), 2)
        result = result + weight * ((1 - bit) if mask & weight else bit)
        weight *= 2
    return result


def kernel(
    sections,
    stream_hbm, query_hbm, key_hbm, value_hbm, incoming_hbm,
    updated_ref, received_ref,
    stream_own, query_own, key_own, value_own,
    query_all, key_all, value_all, result, attended,
    load_sem, own_sem, send_sem, recv_sem, back_send, back_recv, pass_send, pass_recv, first_sem,
):
    section = lax.axis_index("section")
    seq = lax.axis_index("seq")
    me = lax.rem(seq, GROUP)
    base = seq - me
    width = query_all.shape[2]
    masks = list(range(GROUP - 1, 0, -1))
    place = {mask: flipped(me, mask) for mask in range(GROUP)}

    def columns(mask):
        return pl.ds(pl.multiple_of(place[mask] * width, HEAD_SIZE), width)

    sources = (key_hbm, value_hbm, query_hbm)
    held = (key_own, value_own, query_own)
    whole = (key_all, value_all, query_all)
    loads = [pltpu.make_async_copy(sources[i], held[i], load_sem.at[i]) for i in range(3)]
    loads.append(pltpu.make_async_copy(stream_hbm, stream_own, load_sem.at[3]))
    owns = [
        pltpu.make_async_copy(sources[i].at[:, columns(0)], whole[i].at[0], own_sem.at[i])
        for i in range(3)
    ]
    loads[0].start()
    loads[1].start()
    loads[2].start()

    barrier = pltpu.get_barrier_semaphore()
    for mask in masks:
        pl.semaphore_signal(
            barrier, inc=1, device_id={"seq": base + place[mask]}, device_id_type=MESH
        )
    previous = lax.rem(section + sections - 1, sections)
    pl.semaphore_signal(barrier, inc=1, device_id={"section": previous}, device_id_type=MESH)
    for own in owns:
        own.start()
    loads[3].start()
    first = pltpu.make_async_copy(incoming_hbm, received_ref, first_sem)

    @pl.when(section == 0)
    def _():
        first.start()

    def exchange(kind, mask):
        return pltpu.make_async_remote_copy(
            src_ref=held[kind].at[:, columns(mask)],
            dst_ref=whole[kind].at[mask],
            send_sem=send_sem.at[kind, mask],
            recv_sem=recv_sem.at[kind, mask],
            device_id={"seq": base + place[mask]},
            device_id_type=MESH,
        )

    def giving_back(mask):
        return pltpu.make_async_remote_copy(
            src_ref=result.at[mask],
            dst_ref=attended.at[mask],
            send_sem=back_send.at[mask],
            recv_sem=back_recv.at[mask],
            device_id={"seq": base + place[mask]},
            device_id_type=MESH,
        )

    def passing(mask):
        return pltpu.make_async_remote_copy(
            src_ref=updated_ref.at[:, columns(mask)],
            dst_ref=received_ref.at[:, columns(mask)],
            send_sem=pass_send.at[mask],
            recv_sem=pass_recv.at[mask],
            device_id={"section": lax.rem(section + 1, sections)},
            device_id_type=MESH,
        )

    pl.semaphore_wait(barrier, GROUP)
    for kind in range(3):
        loads[kind].wait()
        for mask in masks:
            exchange(kind, mask).start()
    for own in owns:
        own.wait()
    loads[3].wait()
    for kind in range(2):
        for mask in masks:
            exchange(kind, mask).wait_recv()

    factor = HEAD_SIZE ** -0.5 * LOG2_E

    def attend(mask):
        for start in range(0, width, HEAD_SIZE):
            feats = pl.ds(start, HEAD_SIZE)
            keys = key_all[:, :, feats].reshape(-1, HEAD_SIZE)
            vals = value_all[:, :, feats].reshape(-1, HEAD_SIZE)
            scores = lax.dot_general(
                query_all[mask, :, feats], keys, (((1,), (1,)), ((), ())),
                preferred_element_type=jnp.float32,
            )
            highest = jnp.max(scores, axis=-1, keepdims=True)
            exponent = jnp.exp2((scores - highest) * factor)
            totals = jnp.sum(exponent, axis=-1, keepdims=True)
            summed = jnp.dot(
                exponent.astype(jnp.bfloat16), vals, preferred_element_type=jnp.float32
            )
            result[mask, :, feats] = (summed / totals).astype(jnp.bfloat16)

    def update(mask, piece):
        cols = columns(mask)
        updated_ref[:, cols] = (
            stream_own[:, cols].astype(jnp.float32) + piece.astype(jnp.float32)
        ).astype(jnp.bfloat16)

        @pl.when(section < sections - 1)
        def _():
            passing(mask).start()

    attend(0)
    update(0, result[0])
    for mask in masks:
        exchange(2, mask).wait_recv()
        attend(mask)
        giving_back(mask).start()
    for mask in masks:
        giving_back(mask).wait_recv()
        update(mask, attended[mask])

    for mask in masks:
        for kind in range(3):
            exchange(kind, mask).wait_send()
        giving_back(mask).wait_send()

    @pl.when(section < sections - 1)
    def _():
        for mask in range(GROUP):
            passing(mask).wait_send()

    @pl.when(section > 0)
    def _():
        for mask in range(GROUP):
            passing(mask).wait_recv()

    @pl.when(section == 0)
    def _():
        first.wait()


def per_device(sections, stream, queries, key_rows, values, incoming):
    rows, features = incoming.shape
    width = features // GROUP
    block = jax.ShapeDtypeStruct((rows, features), jnp.bfloat16)
    own = pltpu.VMEM((rows, features), jnp.bfloat16)
    whole = pltpu.VMEM((GROUP, rows, width), jnp.bfloat16)
    updated, received = pl.pallas_call(
        functools.partial(kernel, sections),
        out_shape=(block, block),
        in_specs=[pl.BlockSpec(memory_space=pl.ANY)] * 5,
        out_specs=(pl.BlockSpec(memory_space=pltpu.VMEM),) * 2,
        scratch_shapes=[own] * 4 + [whole] * 5 + [
            pltpu.SemaphoreType.DMA((4,)),
            pltpu.SemaphoreType.DMA((3,)),
            pltpu.SemaphoreType.DMA((3, GROUP)),
            pltpu.SemaphoreType.DMA((3, GROUP)),
            pltpu.SemaphoreType.DMA((GROUP,)),
            pltpu.SemaphoreType.DMA((GROUP,)),
            pltpu.SemaphoreType.DMA((GROUP,)),
            pltpu.SemaphoreType.DMA((GROUP,)),
            pltpu.SemaphoreType.DMA,
        ],
        compiler_params=pltpu.CompilerParams(collective_id=0, has_side_effects=True),
    )(stream[0], queries[0], key_rows[0], values[0], incoming)
    return updated[None], received[None]


def solution(mesh):
    placed = (
        P("section", "seq", None),
        P("section", "seq", None),
        P("section", "seq", None),
        P("section", "seq", None),
        P("seq", None),
    )
    return jax.shard_map(
        functools.partial(per_device, mesh.shape["section"]),
        mesh=mesh,
        in_specs=placed,
        out_specs=(P("section", "seq", None), P("section", "seq", None)),
        check_vma=False,
    )
```

```python
import functools

import jax
import jax.numpy as jnp
from jax import lax
from jax.experimental import pallas as pl
from jax.experimental.pallas import tpu as pltpu
from jax.sharding import PartitionSpec as P

HEAD_SIZE = 128
GROUP = 8
LOG2_E = 1.4426950408889634
MESH = pl.DeviceIdType.MESH


def flipped(place, mask):
    result, weight = 0, 1
    while weight < GROUP:
        bit = lax.rem(lax.div(place, weight), 2)
        result = result + weight * ((1 - bit) if mask & weight else bit)
        weight *= 2
    return result


def kernel(
    sections,
    stream_hbm, query_hbm, key_hbm, value_hbm, incoming_hbm,
    both_ref,
    stream_own, query_own, key_own, value_own,
    query_all, key_all, value_all, result, attended,
    load_sem, own_sem, send_sem, recv_sem, back_send, back_recv, pass_send, pass_recv, first_sem,
):
    updated_ref, received_ref = both_ref.at[0], both_ref.at[1]
    section = lax.axis_index("section")
    seq = lax.axis_index("seq")
    me = lax.rem(seq, GROUP)
    base = seq - me
    width = query_all.shape[2]
    masks = list(range(GROUP - 1, 0, -1))
    place = {mask: flipped(me, mask) for mask in range(GROUP)}

    def columns(mask):
        return pl.ds(pl.multiple_of(place[mask] * width, HEAD_SIZE), width)

    sources = (key_hbm, value_hbm, query_hbm)
    held = (key_own, value_own, query_own)
    whole = (key_all, value_all, query_all)
    loads = [pltpu.make_async_copy(sources[i], held[i], load_sem.at[i]) for i in range(3)]
    loads.append(pltpu.make_async_copy(stream_hbm, stream_own, load_sem.at[3]))
    owns = [
        pltpu.make_async_copy(sources[i].at[:, columns(0)], whole[i].at[0], own_sem.at[i])
        for i in range(3)
    ]
    loads[0].start()
    loads[1].start()
    loads[2].start()

    barrier = pltpu.get_barrier_semaphore()
    for mask in masks:
        pl.semaphore_signal(
            barrier, inc=1, device_id={"seq": base + place[mask]}, device_id_type=MESH
        )
    previous = lax.rem(section + sections - 1, sections)
    pl.semaphore_signal(barrier, inc=1, device_id={"section": previous}, device_id_type=MESH)
    for own in owns:
        own.start()
    loads[3].start()
    first = pltpu.make_async_copy(incoming_hbm, received_ref, first_sem)

    @pl.when(section == 0)
    def _():
        first.start()

    def exchange(kind, mask):
        return pltpu.make_async_remote_copy(
            src_ref=held[kind].at[:, columns(mask)],
            dst_ref=whole[kind].at[mask],
            send_sem=send_sem.at[kind, mask],
            recv_sem=recv_sem.at[kind, mask],
            device_id={"seq": base + place[mask]},
            device_id_type=MESH,
        )

    def giving_back(mask):
        return pltpu.make_async_remote_copy(
            src_ref=result.at[mask],
            dst_ref=attended.at[mask],
            send_sem=back_send.at[mask],
            recv_sem=back_recv.at[mask],
            device_id={"seq": base + place[mask]},
            device_id_type=MESH,
        )

    def passing(mask):
        return pltpu.make_async_remote_copy(
            src_ref=updated_ref.at[:, columns(mask)],
            dst_ref=received_ref.at[:, columns(mask)],
            send_sem=pass_send.at[mask],
            recv_sem=pass_recv.at[mask],
            device_id={"section": lax.rem(section + 1, sections)},
            device_id_type=MESH,
        )

    pl.semaphore_wait(barrier, GROUP)
    for kind in range(3):
        loads[kind].wait()
        for mask in masks:
            exchange(kind, mask).start()
    for own in owns:
        own.wait()
    loads[3].wait()
    for kind in range(2):
        for mask in masks:
            exchange(kind, mask).wait_recv()

    factor = HEAD_SIZE ** -0.5 * LOG2_E

    def attend(mask):
        for start in range(0, width, HEAD_SIZE):
            feats = pl.ds(start, HEAD_SIZE)
            keys = key_all[:, :, feats].reshape(-1, HEAD_SIZE)
            vals = value_all[:, :, feats].reshape(-1, HEAD_SIZE)
            scores = lax.dot_general(
                query_all[mask, :, feats], keys, (((1,), (1,)), ((), ())),
                preferred_element_type=jnp.float32,
            )
            highest = jnp.max(scores, axis=-1, keepdims=True)
            exponent = jnp.exp2((scores - highest) * factor)
            totals = jnp.sum(exponent, axis=-1, keepdims=True)
            summed = jnp.dot(
                exponent.astype(jnp.bfloat16), vals, preferred_element_type=jnp.float32
            )
            result[mask, :, feats] = (summed / totals).astype(jnp.bfloat16)

    def update(mask, piece):
        cols = columns(mask)
        updated_ref[:, cols] = (
            stream_own[:, cols].astype(jnp.float32) + piece.astype(jnp.float32)
        ).astype(jnp.bfloat16)

        @pl.when(section < sections - 1)
        def _():
            passing(mask).start()

    attend(0)
    update(0, result[0])
    for mask in masks:
        exchange(2, mask).wait_recv()
        attend(mask)
        giving_back(mask).start()
    for mask in masks:
        giving_back(mask).wait_recv()
        update(mask, attended[mask])

    for mask in masks:
        for kind in range(3):
            exchange(kind, mask).wait_send()
        giving_back(mask).wait_send()

    @pl.when(section < sections - 1)
    def _():
        for mask in range(GROUP):
            passing(mask).wait_send()

    @pl.when(section > 0)
    def _():
        for mask in range(GROUP):
            passing(mask).wait_recv()

    @pl.when(section == 0)
    def _():
        first.wait()


def per_device(sections, stream, queries, key_rows, values, incoming):
    rows, features = incoming.shape
    width = features // GROUP
    block = pltpu.VMEM((2, rows, features), jnp.bfloat16)
    own = pltpu.VMEM((rows, features), jnp.bfloat16)
    whole = pltpu.VMEM((GROUP, rows, width), jnp.bfloat16)
    both = pl.pallas_call(
        functools.partial(kernel, sections),
        out_shape=block,
        in_specs=[pl.BlockSpec(memory_space=pl.ANY)] * 5,
        out_specs=pl.BlockSpec(memory_space=pltpu.VMEM),
        scratch_shapes=[own] * 4 + [whole] * 5 + [
            pltpu.SemaphoreType.DMA((4,)),
            pltpu.SemaphoreType.DMA((3,)),
            pltpu.SemaphoreType.DMA((3, GROUP)),
            pltpu.SemaphoreType.DMA((3, GROUP)),
            pltpu.SemaphoreType.DMA((GROUP,)),
            pltpu.SemaphoreType.DMA((GROUP,)),
            pltpu.SemaphoreType.DMA((GROUP,)),
            pltpu.SemaphoreType.DMA((GROUP,)),
            pltpu.SemaphoreType.DMA,
        ],
        compiler_params=pltpu.CompilerParams(collective_id=0, has_side_effects=True),
    )(stream[0], queries[0], key_rows[0], values[0], incoming)
    return both[:1], both[1:]


def solution(mesh):
    placed = (
        P("section", "seq", None),
        P("section", "seq", None),
        P("section", "seq", None),
        P("section", "seq", None),
        P("seq", None),
    )
    return jax.shard_map(
        functools.partial(per_device, mesh.shape["section"]),
        mesh=mesh,
        in_specs=placed,
        out_specs=(P("section", "seq", None), P("section", "seq", None)),
        check_vma=False,
    )
```

```python
import functools

import jax
import jax.numpy as jnp
from jax import lax
from jax.experimental import pallas as pl
from jax.experimental.pallas import tpu as pltpu
from jax.sharding import PartitionSpec as P

HEAD_SIZE = 128
GROUP = 8
LOG2_E = 1.4426950408889634
MESH = pl.DeviceIdType.MESH


def flipped(place, mask):
    result, weight = 0, 1
    while weight < GROUP:
        bit = lax.rem(lax.div(place, weight), 2)
        result = result + weight * ((1 - bit) if mask & weight else bit)
        weight *= 2
    return result


def kernel(
    sections,
    stream_hbm, query_hbm, key_hbm, value_hbm, incoming_hbm,
    both_ref,
    stream_own, query_own, key_own, value_own,
    query_all, key_all, value_all, result, attended,
    load_sem, own_sem, send_sem, recv_sem, back_send, back_recv, pass_send, pass_recv, first_sem, known_sem,
):
    updated_ref, received_ref = both_ref.at[0], both_ref.at[1]
    section = lax.axis_index("section")
    seq = lax.axis_index("seq")
    me = lax.rem(seq, GROUP)
    base = seq - me
    width = query_all.shape[2]
    masks = [6, 7, 4, 5, 3, 2, 1]
    place = {mask: flipped(me, mask) for mask in range(GROUP)}

    def columns(mask):
        return pl.ds(pl.multiple_of(place[mask] * width, HEAD_SIZE), width)

    sources = (key_hbm, value_hbm, query_hbm)
    held = (key_own, value_own, query_own)
    whole = (key_all, value_all, query_all)
    loads = [pltpu.make_async_copy(sources[i], held[i], load_sem.at[i]) for i in range(3)]
    loads.append(pltpu.make_async_copy(stream_hbm, stream_own, load_sem.at[3]))
    owns = [
        pltpu.make_async_copy(sources[i].at[:, columns(0)], whole[i].at[0], own_sem.at[i])
        for i in range(3)
    ]
    loads[0].start()
    loads[1].start()
    loads[2].start()

    barrier = pltpu.get_barrier_semaphore()
    for mask in (4, 2, 1):
        pl.semaphore_signal(
            barrier, inc=1, device_id={"seq": base + place[mask]}, device_id_type=MESH
        )
    previous = lax.rem(section + sections - 1, sections)
    pl.semaphore_signal(barrier, inc=1, device_id={"section": previous}, device_id_type=MESH)
    for own in owns:
        own.start()
    loads[3].start()
    first = pltpu.make_async_copy(incoming_hbm, received_ref, first_sem)

    @pl.when(section == 0)
    def _():
        first.start()

    def exchange(kind, mask):
        return pltpu.make_async_remote_copy(
            src_ref=held[kind].at[:, columns(mask)],
            dst_ref=whole[kind].at[mask],
            send_sem=send_sem.at[kind, mask],
            recv_sem=recv_sem.at[kind, mask],
            device_id={"seq": base + place[mask]},
            device_id_type=MESH,
        )

    def giving_back(mask):
        return pltpu.make_async_remote_copy(
            src_ref=result.at[mask],
            dst_ref=attended.at[mask],
            send_sem=back_send.at[mask],
            recv_sem=back_recv.at[mask],
            device_id={"seq": base + place[mask]},
            device_id_type=MESH,
        )

    def passing(mask):
        return pltpu.make_async_remote_copy(
            src_ref=updated_ref.at[:, columns(mask)],
            dst_ref=received_ref.at[:, columns(mask)],
            send_sem=pass_send.at[mask],
            recv_sem=pass_recv.at[mask],
            device_id={"section": lax.rem(section + 1, sections)},
            device_id_type=MESH,
        )

    def tell(index, mask):
        pl.semaphore_signal(
            known_sem.at[index], inc=1,
            device_id={"seq": base + place[mask]}, device_id_type=MESH,
        )

    def send(kinds, *to):
        for mask in to:
            for kind in kinds:
                exchange(kind, mask).start()

    pl.semaphore_wait(barrier, 4)
    tell(0, 1)
    tell(1, 2)
    for kind in range(3):
        loads[kind].wait()
    send((0, 1), 4, 1)
    pl.semaphore_wait(known_sem.at[0], 1)
    send((0, 1), 5)
    pl.semaphore_wait(known_sem.at[1], 1)
    tell(2, 1)
    send((0, 1), 6, 2)
    pl.semaphore_wait(known_sem.at[2], 1)
    send((0, 1), 7, 3)
    send((2,), *masks)
    for own in owns:
        own.wait()
    loads[3].wait()
    for kind in range(2):
        for mask in masks:
            exchange(kind, mask).wait_recv()

    factor = HEAD_SIZE ** -0.5 * LOG2_E

    def attend(mask):
        for start in range(0, width, HEAD_SIZE):
            feats = pl.ds(start, HEAD_SIZE)
            keys = key_all[:, :, feats].reshape(-1, HEAD_SIZE)
            vals = value_all[:, :, feats].reshape(-1, HEAD_SIZE)
            scores = lax.dot_general(
                query_all[mask, :, feats], keys, (((1,), (1,)), ((), ())),
                preferred_element_type=jnp.float32,
            )
            highest = jnp.max(scores, axis=-1, keepdims=True)
            exponent = jnp.exp2((scores - highest) * factor)
            totals = jnp.sum(exponent, axis=-1, keepdims=True)
            summed = jnp.dot(
                exponent.astype(jnp.bfloat16), vals, preferred_element_type=jnp.float32
            )
            result[mask, :, feats] = (summed / totals).astype(jnp.bfloat16)

    def update(mask, piece):
        cols = columns(mask)
        updated_ref[:, cols] = (
            stream_own[:, cols].astype(jnp.float32) + piece.astype(jnp.float32)
        ).astype(jnp.bfloat16)

        @pl.when(section < sections - 1)
        def _():
            passing(mask).start()

    for mask in masks:
        exchange(2, mask).wait_recv()
        attend(mask)
        giving_back(mask).start()
        if mask == masks[6]:
            attend(0)
            update(0, result[0])
    for mask in masks:
        giving_back(mask).wait_recv()
        update(mask, attended[mask])

    for mask in masks:
        for kind in range(3):
            exchange(kind, mask).wait_send()
        giving_back(mask).wait_send()

    @pl.when(section < sections - 1)
    def _():
        for mask in range(GROUP):
            passing(mask).wait_send()

    @pl.when(section > 0)
    def _():
        for mask in range(GROUP):
            passing(mask).wait_recv()

    @pl.when(section == 0)
    def _():
        first.wait()


def per_device(sections, stream, queries, key_rows, values, incoming):
    rows, features = incoming.shape
    width = features // GROUP
    block = pltpu.VMEM((2, rows, features), jnp.bfloat16)
    own = pltpu.VMEM((rows, features), jnp.bfloat16)
    whole = pltpu.VMEM((GROUP, rows, width), jnp.bfloat16)
    both = pl.pallas_call(
        functools.partial(kernel, sections),
        out_shape=block,
        in_specs=[pl.BlockSpec(memory_space=pl.ANY)] * 5,
        out_specs=pl.BlockSpec(memory_space=pltpu.VMEM),
        scratch_shapes=[own] * 4 + [whole] * 5 + [
            pltpu.SemaphoreType.DMA((4,)),
            pltpu.SemaphoreType.DMA((3,)),
            pltpu.SemaphoreType.DMA((3, GROUP)),
            pltpu.SemaphoreType.DMA((3, GROUP)),
            pltpu.SemaphoreType.DMA((GROUP,)),
            pltpu.SemaphoreType.DMA((GROUP,)),
            pltpu.SemaphoreType.DMA((GROUP,)),
            pltpu.SemaphoreType.DMA((GROUP,)),
            pltpu.SemaphoreType.DMA,
            pltpu.SemaphoreType.REGULAR((3,)),
        ],
        compiler_params=pltpu.CompilerParams(collective_id=0, has_side_effects=True),
    )(stream[0], queries[0], key_rows[0], values[0], incoming)
    return both[:1], both[1:]


def solution(mesh):
    placed = (
        P("section", "seq", None),
        P("section", "seq", None),
        P("section", "seq", None),
        P("section", "seq", None),
        P("seq", None),
    )
    return jax.shard_map(
        functools.partial(per_device, mesh.shape["section"]),
        mesh=mesh,
        in_specs=placed,
        out_specs=(P("section", "seq", None), P("section", "seq", None)),
        check_vma=False,
    )
```

```python
import functools

import jax
import jax.numpy as jnp
from jax import lax
from jax.experimental import pallas as pl
from jax.experimental.pallas import tpu as pltpu
from jax.sharding import PartitionSpec as P

HEAD_SIZE = 128
GROUP = 8
LOG2_E = 1.4426950408889634
MESH = pl.DeviceIdType.MESH


def flipped(place, mask):
    result, weight = 0, 1
    while weight < GROUP:
        bit = lax.rem(lax.div(place, weight), 2)
        result = result + weight * ((1 - bit) if mask & weight else bit)
        weight *= 2
    return result


def kernel(
    sections,
    stream_hbm, query_hbm, key_hbm, value_hbm, incoming_hbm,
    both_ref,
    stream_own, query_own, key_own, value_own,
    query_all, key_all, value_all, result, attended,
    load_sem, own_sem, send_sem, recv_sem, back_send, back_recv, pass_send, pass_recv, first_sem, known_sem,
):
    updated_ref, received_ref = both_ref.at[0], both_ref.at[1]
    section = lax.axis_index("section")
    seq = lax.axis_index("seq")
    me = lax.rem(seq, GROUP)
    base = seq - me
    width = query_all.shape[2]
    masks = [1, 6, 7, 4, 5, 3, 2]
    place = {mask: flipped(me, mask) for mask in range(GROUP)}

    def columns_of(partner):
        return pl.ds(pl.multiple_of((partner - base) * width, HEAD_SIZE), width)

    def columns(mask):
        return pl.ds(pl.multiple_of(place[mask] * width, HEAD_SIZE), width)

    sources = (key_hbm, value_hbm, query_hbm)
    held = (key_own, value_own, query_own)
    whole = (key_all, value_all, query_all)
    loads = [pltpu.make_async_copy(sources[i], held[i], load_sem.at[i]) for i in range(3)]
    loads.append(pltpu.make_async_copy(stream_hbm, stream_own, load_sem.at[3]))
    owns = [
        pltpu.make_async_copy(sources[i].at[:, columns(0)], whole[i].at[0], own_sem.at[i])
        for i in range(3)
    ]
    loads[0].start()
    loads[1].start()
    loads[2].start()

    barrier = pltpu.get_barrier_semaphore()
    for mask in (4, 2, 1):
        pl.semaphore_signal(
            barrier, inc=1, device_id={"seq": base + place[mask]}, device_id_type=MESH
        )
    previous = lax.rem(section + sections - 1, sections)
    pl.semaphore_signal(barrier, inc=1, device_id={"section": previous}, device_id_type=MESH)
    for own in owns:
        own.start()
    loads[3].start()
    first = pltpu.make_async_copy(incoming_hbm, received_ref, first_sem)

    @pl.when(section == 0)
    def _():
        first.start()

    def exchange(kind, mask, partner=None):
        partner = base + place[mask] if partner is None else partner
        return pltpu.make_async_remote_copy(
            src_ref=held[kind].at[:, columns_of(partner)],
            dst_ref=whole[kind].at[mask],
            send_sem=send_sem.at[kind, mask],
            recv_sem=recv_sem.at[kind, mask],
            device_id={"seq": partner},
            device_id_type=MESH,
        )

    def giving_back(mask, partner=None):
        partner = base + place[mask] if partner is None else partner
        return pltpu.make_async_remote_copy(
            src_ref=result.at[mask],
            dst_ref=attended.at[mask],
            send_sem=back_send.at[mask],
            recv_sem=back_recv.at[mask],
            device_id={"seq": partner},
            device_id_type=MESH,
        )

    def passing(mask):
        return pltpu.make_async_remote_copy(
            src_ref=updated_ref.at[:, columns(mask)],
            dst_ref=received_ref.at[:, columns(mask)],
            send_sem=pass_send.at[mask],
            recv_sem=pass_recv.at[mask],
            device_id={"section": lax.rem(section + 1, sections)},
            device_id_type=MESH,
        )

    def tell(index, mask):
        pl.semaphore_signal(
            known_sem.at[index], inc=1,
            device_id={"seq": base + place[mask]}, device_id_type=MESH,
        )

    def send(kinds, *to):
        for mask in to:
            for kind in kinds:
                exchange(kind, mask).start()

    pl.semaphore_wait(barrier, 4)
    tell(0, 1)
    tell(1, 2)
    for kind in range(3):
        loads[kind].wait()
    send((0, 1), 4, 1)
    pl.semaphore_wait(known_sem.at[0], 1)
    send((0, 1), 5)
    pl.semaphore_wait(known_sem.at[1], 1)
    tell(2, 1)
    send((0, 1), 6)
    pl.semaphore_wait(known_sem.at[2], 1)
    send((0, 1), 7, 3, 2)
    send((2,), *masks)
    for own in owns:
        own.wait()
    loads[3].wait()
    for kind in range(2):
        for mask in masks:
            exchange(kind, mask).wait_recv()

    factor = HEAD_SIZE ** -0.5 * LOG2_E

    def attend(mask):
        for start in range(0, width, HEAD_SIZE):
            feats = pl.ds(start, HEAD_SIZE)
            keys = key_all[:, :, feats].reshape(-1, HEAD_SIZE)
            vals = value_all[:, :, feats].reshape(-1, HEAD_SIZE)
            scores = lax.dot_general(
                query_all[mask, :, feats], keys, (((1,), (1,)), ((), ())),
                preferred_element_type=jnp.float32,
            )
            highest = jnp.max(scores, axis=-1, keepdims=True)
            exponent = jnp.exp2((scores - highest) * factor)
            totals = jnp.sum(exponent, axis=-1, keepdims=True)
            summed = jnp.dot(
                exponent.astype(jnp.bfloat16), vals, preferred_element_type=jnp.float32
            )
            result[mask, :, feats] = (summed * (1.0 / totals)).astype(jnp.bfloat16)

    def update(mask, piece):
        cols = columns(mask)
        updated_ref[:, cols] = (
            stream_own[:, cols].astype(jnp.float32) + piece.astype(jnp.float32)
        ).astype(jnp.bfloat16)

        @pl.when(section < sections - 1)
        def _():
            passing(mask).start()

    def serve(mask, partner):
        exchange(2, mask, partner).wait_recv()
        attend(mask)
        giving_back(mask, partner).start()

    @pl.when(me > 0)
    def _():
        serve(me, base)

    for mask in masks:

        @pl.when(me != mask)
        def _():
            serve(mask, base + place[mask])

    attend(0)
    update(0, result[0])
    for mask in masks:
        giving_back(mask).wait_recv()
        update(mask, attended[mask])

    for mask in masks:
        for kind in range(3):
            exchange(kind, mask).wait_send()
        giving_back(mask).wait_send()

    @pl.when(section < sections - 1)
    def _():
        for mask in range(GROUP):
            passing(mask).wait_send()

    @pl.when(section > 0)
    def _():
        for mask in range(GROUP):
            passing(mask).wait_recv()

    @pl.when(section == 0)
    def _():
        first.wait()


def per_device(sections, stream, queries, key_rows, values, incoming):
    rows, features = incoming.shape
    width = features // GROUP
    block = pltpu.VMEM((2, rows, features), jnp.bfloat16)
    own = pltpu.VMEM((rows, features), jnp.bfloat16)
    whole = pltpu.VMEM((GROUP, rows, width), jnp.bfloat16)
    both = pl.pallas_call(
        functools.partial(kernel, sections),
        out_shape=block,
        in_specs=[pl.BlockSpec(memory_space=pl.ANY)] * 5,
        out_specs=pl.BlockSpec(memory_space=pltpu.VMEM),
        scratch_shapes=[own] * 4 + [whole] * 5 + [
            pltpu.SemaphoreType.DMA((4,)),
            pltpu.SemaphoreType.DMA((3,)),
            pltpu.SemaphoreType.DMA((3, GROUP)),
            pltpu.SemaphoreType.DMA((3, GROUP)),
            pltpu.SemaphoreType.DMA((GROUP,)),
            pltpu.SemaphoreType.DMA((GROUP,)),
            pltpu.SemaphoreType.DMA((GROUP,)),
            pltpu.SemaphoreType.DMA((GROUP,)),
            pltpu.SemaphoreType.DMA,
            pltpu.SemaphoreType.REGULAR((3,)),
        ],
        compiler_params=pltpu.CompilerParams(collective_id=0, has_side_effects=True),
    )(stream[0], queries[0], key_rows[0], values[0], incoming)
    return both[:1], both[1:]


def solution(mesh):
    placed = (
        P("section", "seq", None),
        P("section", "seq", None),
        P("section", "seq", None),
        P("section", "seq", None),
        P("seq", None),
    )
    return jax.shard_map(
        functools.partial(per_device, mesh.shape["section"]),
        mesh=mesh,
        in_specs=placed,
        out_specs=(P("section", "seq", None), P("section", "seq", None)),
        check_vma=False,
    )
```
